32 devices in a mesh: modes: 8 (over z, y), cheb: 4 (over x, core).
Axes of the slice: x: 2, y: 2, z: 4, core: 2. Of those that a mesh axis runs over, the one named last changes fastest.
Arguments:
- start: float32 [2, 2, 2048, 256], P(None, None, ('modes', 'cheb')), may hold values from -45 to 45
- forcing: float32 [2, 2, 2048, 256], P(None, None, ('modes', 'cheb')), may hold values from -45 to 45
- taus: float32 [2048, 256, 256], P(('modes', 'cheb')), may hold values from -5 to 5
Outputs:
- solution: float32 [2, 2, 2048, 256], P(None, None, ('modes', 'cheb'))
The draws below stay inside these ranges and needn't reach their ends.
All inputs are finite; a program needn't handle non-finite values.
Results may differ from the reference program's by a relative error of at most 0.0002.
Values sent between devices are 32-bit elements; how exact they have to be, the bound alone decides.
No kernel may reach another device: no remote copies, remote signals or barrier semaphores. Data moves between devices by JAX's collectives and lax.ppermute only.
A program may use at most 128 MiB of HBM per device.

```python
import math
import jax
import jax.numpy as jnp
from jax import lax

KX = 2048
NY = 256
BATCH = 2
NEWTON = 2
KRYLOV = 3


def spectral_field(key):
    subkeys = jax.random.split(key, 3)
    entries = jnp.clip(jax.random.normal(subkeys[0], (BATCH, 2, KX, NY), jnp.float32), -5.0, 5.0)
    log_low = math.log(0.3)
    log_high = math.log(3.0)
    mode_scale = jnp.exp(jax.random.uniform(subkeys[1], (1, 1, KX, 1), jnp.float32, log_low, log_high))
    degree_scale = jnp.exp(jax.random.uniform(subkeys[2], (1, 1, 1, NY), jnp.float32, log_low, log_high))
    return entries * mode_scale * degree_scale


def draw_start(key, part):
    return spectral_field(jax.random.fold_in(key, 11))


def draw_forcing(key, part):
    return spectral_field(jax.random.fold_in(key, 23))


def draw_taus(key, part):
    subkeys = jax.random.split(jax.random.fold_in(key, 37), 3)
    wavenumber = 16.0 * jnp.arange(KX, dtype=jnp.int32).astype(jnp.float32) / KX
    envelope = 1.0 / (1.0 + wavenumber * wavenumber / 16.0)
    rough = jnp.exp(jax.random.uniform(subkeys[0], (KX,), jnp.float32, math.log(0.5), math.log(2.0)))
    diagonal = jnp.exp(jax.random.uniform(subkeys[1], (KX, NY), jnp.float32, math.log(0.5), math.log(2.0)))
    offdiag = jnp.clip(jax.random.normal(subkeys[2], (KX, NY, NY), jnp.float32), -5.0, 5.0)
    matrix = offdiag * (0.3 / math.sqrt(NY)) + diagonal[:, :, None] * jnp.eye(NY, dtype=jnp.float32)[None, :, :]
    return matrix * (envelope * rough)[:, None, None]


def setup_inputs(seed: int = 0) -> dict:
    streams_of = jax.random.split(jax.random.key(seed), 4)
    return {
        "start": draw_start(jax.random.fold_in(streams_of[3], 71), 0),
        "forcing": draw_forcing(jax.random.fold_in(streams_of[3], 71), 0),
        "taus": draw_taus(jax.random.fold_in(streams_of[3], 71), 0),
    }


HIGH = lax.Precision.HIGHEST
STRENGTH = 0.1

def cheb_rows(degree_count):
    degree = jnp.arange(degree_count, dtype=jnp.int32)[:, None]
    node = 2 * jnp.arange(degree_count, dtype=jnp.int32)[None, :] + 1
    turns = degree * node % (4 * degree_count)
    return jnp.cos(2.0 * math.pi / (4 * degree_count) * turns.astype(jnp.float32))

def sample_grid(values):
    spectrum = lax.complex(values[:, 0], values[:, 1])
    spectrum = jnp.concatenate([spectrum, jnp.zeros_like(spectrum[:, :1])], axis=1)
    return jnp.fft.irfft(spectrum, n=2 * KX, axis=1) * (2 * KX / math.sqrt(KX * NY))

def to_points(coefs, cheb_table):
    values = jnp.einsum('brkn,ni->brki', coefs, cheb_table, precision=HIGH)
    wavenumber = (16.0 * jnp.arange(KX, dtype=jnp.int32).astype(jnp.float32) / KX)[:, None]
    slopes = jnp.stack([-wavenumber * values[:, 1], wavenumber * values[:, 0]], axis=1)
    return (sample_grid(values), sample_grid(slopes))

def to_coefficients(points, cheb_table):
    spectrum = jnp.fft.rfft(points, axis=1)[:, :KX] / (2 * KX)
    parts = jnp.stack([jnp.real(spectrum), jnp.imag(spectrum)], axis=1).astype(points.dtype)
    weights = (jnp.where(jnp.arange(NY) == 0, 1.0, 2.0) / NY).astype(points.dtype)
    coefs = jnp.einsum('brki,ni->brkn', parts, cheb_table, precision=HIGH)
    return coefs * weights * math.sqrt(KX * NY)

def precondition(coefs, taus):
    tau_keep = (jnp.arange(NY) < NY - 2).astype(coefs.dtype)
    return jnp.einsum('kam,brkm->brka', taus, coefs * tau_keep, precision=HIGH)

def least_squares(hessen, beta_norm):
    steps_count = len(hessen)
    matrix = [[hessen[col_index][:, row_index] for row_index in range(col_index + 2)] for col_index in range(steps_count)]
    target = [beta_norm] + [jnp.zeros_like(beta_norm) for row_index in range(steps_count)]
    cosines = []
    sines_list = []
    for col_index in range(steps_count):
        column = matrix[col_index]
        for row_index in range(col_index):
            upper_entry = cosines[row_index] * column[row_index] + sines_list[row_index] * column[row_index + 1]
            lower_entry = cosines[row_index] * column[row_index + 1] - sines_list[row_index] * column[row_index]
            column[row_index] = upper_entry
            column[row_index + 1] = lower_entry
        radius = jnp.sqrt(column[col_index] * column[col_index] + column[col_index + 1] * column[col_index + 1])
        cosines.append(column[col_index] / radius)
        sines_list.append(column[col_index + 1] / radius)
        column[col_index] = radius
        target[col_index + 1] = -sines_list[col_index] * target[col_index]
        target[col_index] = cosines[col_index] * target[col_index]
    solved = [None] * steps_count
    for row_index in reversed(range(steps_count)):
        partial_sum = target[row_index]
        for col_index in range(row_index + 1, steps_count):
            partial_sum = partial_sum - matrix[col_index][row_index] * solved[col_index]
        solved[row_index] = partial_sum / matrix[row_index][row_index]
    return solved

def reference(start, forcing, taus):
    cheb_table = cheb_rows(NY)
    iterate = start
    for newton_step in range(NEWTON):
        base_points, base_slopes = to_points(iterate, cheb_table)
        residual = iterate + precondition(to_coefficients(STRENGTH * base_points * base_slopes, cheb_table) - forcing, taus)
        beta_norm = jnp.sqrt(lax.optimization_barrier(jnp.sum(residual * residual, axis=(1, 2, 3))))
        krylov_basis = [-residual / beta_norm[:, None, None, None]]
        hessen = []
        for column in range(KRYLOV):
            probe_points, probe_slopes = to_points(krylov_basis[column], cheb_table)
            product = STRENGTH * (base_points * probe_slopes + probe_points * base_slopes)
            applied = krylov_basis[column] + precondition(to_coefficients(product, cheb_table), taus)
            projections = jnp.stack([lax.optimization_barrier(jnp.sum(vector * applied, axis=(1, 2, 3))) for vector in krylov_basis], axis=1)
            for index, vector in enumerate(krylov_basis):
                applied = applied - projections[:, index][:, None, None, None] * vector
            length = jnp.sqrt(lax.optimization_barrier(jnp.sum(applied * applied, axis=(1, 2, 3))))
            hessen.append(jnp.concatenate([projections, length[:, None]], axis=1))
            krylov_basis.append(applied / length[:, None, None, None])
        solved = least_squares(hessen, beta_norm)
        for column in range(KRYLOV):
            iterate = iterate + solved[column][:, None, None, None] * krylov_basis[column]
    return iterate
```

```python
import math

import jax
import jax.numpy as jnp
import numpy as np
from jax import lax
from jax.experimental import pallas as pl
from jax.experimental.pallas import tpu as pltpu
from jax.sharding import PartitionSpec as P

NEWTON = 2
KRYLOV = 3
STRENGTH = 0.1
AXES = ("modes", "cheb")
F32 = jnp.float32
BF16 = jnp.bfloat16
DOTS = 8


def halves(table):
    table = np.asarray(table, np.float32)
    high = table.astype(BF16)
    low = (table - high.astype(np.float32)).astype(BF16)
    return np.stack([high, low])


def split(x):
    high = x.astype(BF16)
    return high, (x - high.astype(F32)).astype(BF16)


def mm(a, b):
    return lax.dot_general(a, b, (((1,), (0,)), ((), ())), preferred_element_type=F32)


def table_left(t_ref, x):
    high, low = split(x)
    return mm(t_ref[0], high) + (mm(t_ref[0], low) + mm(t_ref[1], high))


def table_right(x, t_ref):
    high, low = split(x)
    return mm(high, t_ref[0]) + (mm(low, t_ref[0]) + mm(high, t_ref[1]))


def least_squares(hessen, beta_norm):
    steps_count = len(hessen)
    matrix = [list(column) for column in hessen]
    target = [beta_norm] + [jnp.zeros_like(beta_norm)] * steps_count
    cosines = []
    sines = []
    for col in range(steps_count):
        column = matrix[col]
        for row in range(col):
            upper = cosines[row] * column[row] + sines[row] * column[row + 1]
            lower = cosines[row] * column[row + 1] - sines[row] * column[row]
            column[row] = upper
            column[row + 1] = lower
        radius = jnp.sqrt(column[col] * column[col] + column[col + 1] * column[col + 1])
        cosines.append(column[col] / radius)
        sines.append(column[col + 1] / radius)
        column[col] = radius
        target[col + 1] = -sines[col] * target[col]
        target[col] = cosines[col] * target[col]
    solved = [None] * steps_count
    for row in reversed(range(steps_count)):
        partial = target[row]
        for col in range(row + 1, steps_count):
            partial = partial - matrix[col][row] * solved[col]
        solved[row] = partial / matrix[row][row]
    return solved


class Plan:
    def __init__(self, group, batch, kl, ny):
        self.group, self.batch, self.kl, self.ny = group, batch, kl, ny
        self.il = ny // group
        self.bq = batch * kl
        self.j1 = 2 * group
        self.direct = self.il % 8 == 0 and self.bq % 128 == 0
        modes = kl * group
        points = 2 * modes
        spread = 1.0 / math.sqrt(modes * ny)
        tau = 2.0 * np.pi
        n, i = np.arange(ny)[:, None], np.arange(ny)[None, :]
        cheb = np.cos(tau / (4 * ny) * (n * (2 * i + 1) % (4 * ny)))
        self.ct = halves(cheb.T)
        self.cw = halves(cheb * (np.where(n == 0, 1.0, 2.0) / ny))
        d, j = np.arange(group)[None, :], np.arange(self.j1)[:, None]
        angle = tau / self.j1 * (d * j % self.j1)
        co, si = np.cos(angle), np.sin(angle)
        slope = 16.0 / modes * kl * d
        self.t1 = halves(np.block([
            [co, -si], [si, co], [-slope * si, -slope * co], [slope * co, -slope * si],
        ]))
        scale = STRENGTH / (spread * points)
        self.t4 = halves(scale * np.block([[co.T, si.T], [-si.T, co.T]]))
        q = np.arange(kl)
        twist = tau / points * (j * q[None, :] % points)
        slope_q = np.broadcast_to(16.0 / modes * q[None, :], twist.shape)
        self.tw = np.stack([
            np.tile(t, (1, batch)) for t in (np.cos(twist), np.sin(twist), slope_q)
        ]).astype(np.float32)
        weight = np.full((group, kl), 2.0 * spread)
        weight[0, 0] = spread
        self.wt = np.tile(weight, (2, batch)).astype(np.float32)
        inner = tau / kl * (q[:, None] * q[None, :] % kl)
        eye = np.eye(batch)
        self.b2 = halves(np.concatenate([np.kron(eye, np.cos(inner)), np.kron(eye, -np.sin(inner))], 0))
        self.b3 = halves(np.concatenate([np.kron(eye, np.cos(inner)), np.kron(eye, -np.sin(inner))], 1))
        self.ones = np.kron(eye, np.ones((kl, kl))).astype(np.float32)

    def tables(self):
        return [self.t1, self.tw, self.wt, self.b2, self.b3, self.t4, self.ones]


def flow_sums(dots, ones_ref):
    total = jnp.sum(dots, axis=0)
    return jnp.dot(total, ones_ref[...], precision=lax.Precision.HIGHEST, preferred_element_type=F32)


def new_column(sums, count):
    heads = [sums[i : i + 1] for i in range(count)]
    square = sums[count : count + 1]
    for head in heads:
        square = square - head * head
    return heads + [jnp.sqrt(square)]


def solve_rows(sums, scal):
    hessen = [[s[i : i + 1] for i in range(n + 2)] for n, s in enumerate(scal[1:])]
    hessen.append(new_column(sums, KRYLOV))
    return least_squares(hessen, scal[0][0:1])


def put_rows(ref, rows):
    ref[...] = jnp.zeros(ref.shape, F32)
    for index, row in enumerate(rows):
        ref[index : index + 1, :] = row


def points_call(plan, mode, field=None, dots=None, base=None, basis=(), scal=()):
    group, il, bq, j1 = plan.group, plan.il, plan.bq, plan.j1
    stride_in, stride_out = 2 * il + DOTS, 2 * il
    names, args = [], []

    def add(name, value):
        names.append(name)
        args.append(value)

    for name, value in zip(("t1", "tw", "wt", "b2", "b3", "t4", "ones"), plan.tables()):
        add(name, jnp.asarray(value))
    if field is not None:
        add("field", field)
    if dots is not None:
        add("dots", dots)
    if base is not None:
        add("base", base)
    for i, v in enumerate(basis):
        add(f"v{i}", v)
    for i, v in enumerate(scal):
        add(f"s{i}", v)
    pts_shape = jax.ShapeDtypeStruct((il, 2, j1, bq), F32)
    if plan.direct:
        send_shape = jax.ShapeDtypeStruct((group * stride_out, bq), F32)
    else:
        send_shape = jax.ShapeDtypeStruct((2 * group, il * bq), F32)
    outs = [send_shape, pts_shape]
    if mode != "start":
        outs.append(jax.ShapeDtypeStruct((DOTS, bq), F32))

    def kernel(*refs):
        ins = dict(zip(names, refs[: len(names)]))
        send, pts_out = refs[len(names)], refs[len(names) + 1]
        rows_out = refs[len(names) + 2] if mode != "start" else None

        def to_points():
            if plan.direct:
                sides = [
                    jnp.concatenate(
                        [ins["field"][pl.ds(r * il + i, group, stride=stride_in), :] for i in range(il)],
                        axis=1,
                    )
                    for r in range(2)
                ]
                x = jnp.concatenate(sides, axis=0)
            else:
                x = ins["field"][...]
            x = x * jnp.concatenate([ins["wt"][...]] * il, axis=1)
            z = table_left(ins["t1"], x)
            co, si, gq = ins["tw"][0], ins["tw"][1], ins["tw"][2]
            rows = []
            for i in range(il):
                part = z[:, i * bq : (i + 1) * bq]
                re, im = part[:j1], part[j1 : 2 * j1]
                sre = part[2 * j1 : 3 * j1] - gq * im
                sim = part[3 * j1 :] + gq * re
                for a, b in ((re, im), (sre, sim)):
                    rows.append(jnp.concatenate([a * co - b * si, a * si + b * co], axis=1))
            return table_right(jnp.concatenate(rows, axis=0), ins["b2"]).reshape(il, 2, j1, bq)

        if mode == "start":
            pts = to_points()
            pts_out[...] = pts
            product = pts[:, 0] * pts[:, 1]
        elif mode == "basis":
            if plan.direct:
                parts = ins["field"][...].reshape(group, stride_in, bq)[:, 2 * il :, :]
            else:
                parts = ins["dots"][...]
            sums = flow_sums(parts, ins["ones"])
            pts = to_points()
            if not basis:
                column = [jnp.sqrt(sums[0:1])]
                pts = pts * (-1.0 / column[0])
            else:
                column = new_column(sums, len(basis))
                for i in range(len(basis)):
                    pts = pts - column[i] * ins[f"v{i}"][...]
                pts = pts * (1.0 / column[-1])
            put_rows(rows_out, column)
            pts_out[...] = pts
            product = ins["base"][:, 0] * pts[:, 1] + pts[:, 0] * ins["base"][:, 1]
        else:
            sums = flow_sums(ins["dots"][...], ins["ones"])
            solved = solve_rows(sums, [ins[f"s{i}"][...] for i in range(KRYLOV)])
            pts = ins["base"][...]
            for i in range(KRYLOV):
                pts = pts + solved[i] * ins[f"v{i}"][...]
            put_rows(rows_out, solved)
            pts_out[...] = pts
            product = pts[:, 0] * pts[:, 1]
        part = table_right(product.reshape(il * j1, bq), ins["b3"])
        co, si = ins["tw"][0], ins["tw"][1]
        cols = []
        for i in range(il):
            re, im = part[i * j1 : (i + 1) * j1, :bq], part[i * j1 : (i + 1) * j1, bq:]
            cols.append(jnp.concatenate([re * co + im * si, im * co - re * si], axis=0))
        out = table_left(ins["t4"], jnp.concatenate(cols, axis=1))
        if plan.direct:
            for r in range(2):
                for i in range(il):
                    send[pl.ds(r * il + i, group, stride=stride_out), :] = out[
                        r * group : (r + 1) * group, i * bq : (i + 1) * bq
                    ]
        else:
            send[...] = out

    return pl.pallas_call(kernel, out_shape=outs, name=f"points_{mode}_{len(basis)}")(*args)


def spectral_call(plan, mode, recv, taus, states, basis=(), scal=None, emit=True):
    group, il, bq, ny, kl = plan.group, plan.il, plan.bq, plan.ny, plan.kl
    wide = 2 * bq
    qb = min(8, kl)
    steps = kl // qb
    lines = wide
    names, args, specs = [], [], []

    def add(name, value):
        names.append(name)
        args.append(value)
        rank = value.ndim
        specs.append(pl.BlockSpec(value.shape, lambda s, rank=rank: (0,) * rank))

    add("recv", recv)
    add("ct", jnp.asarray(plan.ct))
    add("cw", jnp.asarray(plan.cw))
    for i, v in enumerate(states):
        add(f"x{i}", v)
    for i, v in enumerate(basis):
        add(f"v{i}", v)
    if scal is not None:
        add("scal", scal)
    names.append("taus")
    args.append(taus)
    specs.append(pl.BlockSpec((qb, ny, ny), lambda s: (s, 0, 0)))

    state_shape = jax.ShapeDtypeStruct((ny, wide), F32)
    out_names, outs = [], []
    if mode == "residual":
        if basis:
            out_names.append("iterate")
            outs.append(state_shape)
    else:
        out_names.append("vector")
        outs.append(state_shape)
    if emit:
        out_names.append("applied")
        outs.append(state_shape)
        out_names.append("send")
        if plan.direct:
            outs.append(jax.ShapeDtypeStruct((group, 2 * il + DOTS, bq), F32))
        else:
            outs.append(jax.ShapeDtypeStruct((2, ny, bq), F32))
    if not (emit and plan.direct):
        out_names.append("dots")
        outs.append(jax.ShapeDtypeStruct((DOTS, bq), F32))
    out_specs = [
        pl.BlockSpec(o.shape, lambda s, rank=len(o.shape): (0,) * rank) for o in outs
    ]

    def kernel(*refs):
        ins = dict(zip(names, refs[: len(names)]))
        res = dict(zip(out_names, refs[len(names) : len(names) + len(outs)]))
        c_scr, m_scr = refs[len(names) + len(outs) :]
        step = pl.program_id(0)

        @pl.when(step == 0)
        def _():
            if plan.direct:
                sides = [
                    ins["recv"][:, r * il : (r + 1) * il, :].reshape(ny, bq) for r in range(2)
                ]
            else:
                sides = [ins["recv"][r] for r in range(2)]
            coef = table_left(ins["cw"], jnp.concatenate(sides, axis=1))
            if mode == "residual":
                coef = coef - ins["x1"][...]
            degree = lax.broadcasted_iota(jnp.int32, coef.shape, 0)
            coef = jnp.where(degree < ny - 2, coef, 0.0).T
            high = coef.astype(BF16).astype(F32)
            for h in range(ny // 128):
                c_scr[h, :lines, :] = high[:, h * 128 : (h + 1) * 128]
                c_scr[h, lines:, :] = (coef - high)[:, h * 128 : (h + 1) * 128]

        for t in range(qb):
            q = step * qb + t
            picked = pl.ds(q, 2 * lines // kl, stride=kl)
            rows = jnp.concatenate([c_scr[h, picked, :] for h in range(ny // 128)], axis=1).astype(BF16)
            high, low = split(ins["taus"][t])
            dims = (((1,), (1,)), ((), ()))
            got = lax.dot_general(rows, high, dims, preferred_element_type=F32)
            got = got + lax.dot_general(rows, low, dims, preferred_element_type=F32)
            for h in range(ny // 128):
                m_scr[h, picked, :] = got[:, h * 128 : (h + 1) * 128]

        @pl.when(step == steps - 1)
        def _():
            mapped = jnp.concatenate(
                [m_scr[h, :lines, :] + m_scr[h, lines:, :] for h in range(ny // 128)], axis=1
            ).T

            def row(index):
                r = ins["scal"][index : index + 1, :]
                return jnp.concatenate([r, r], axis=1)

            vector = ins["x0"][...]
            if mode == "residual":
                if basis:
                    for i in range(len(basis)):
                        vector = vector + row(i) * ins[f"v{i}"][...]
                    res["iterate"][...] = vector
                others = []
            else:
                if not basis:
                    vector = vector * (-1.0 / row(0))
                else:
                    for i in range(len(basis)):
                        vector = vector - row(i) * ins[f"v{i}"][...]
                    vector = vector * (1.0 / row(len(basis)))
                res["vector"][...] = vector
                others = [ins[f"v{i}"][...] for i in range(len(basis))] + [vector]
            applied = vector + mapped
            lanes = []
            for other in others + [applied]:
                dot = jnp.sum(other * applied, axis=0, keepdims=True)
                lanes.append(dot[:, :bq] + dot[:, bq:])
            lanes += [jnp.zeros((1, bq), F32)] * (DOTS - len(lanes))
            dots = jnp.concatenate(lanes, axis=0)
            if emit:
                res["applied"][...] = applied
                values = table_left(ins["ct"], applied)
                for r in range(2):
                    side = values[:, r * bq : (r + 1) * bq]
                    if plan.direct:
                        res["send"][:, r * il : (r + 1) * il, :] = side.reshape(group, il, bq)
                    else:
                        res["send"][r] = side
            if emit and plan.direct:
                res["send"][:, 2 * il :, :] = jnp.broadcast_to(dots[None], (group, DOTS, bq))
            else:
                res["dots"][...] = dots

    got = pl.pallas_call(
        kernel,
        grid=(steps,),
        in_specs=specs,
        out_specs=out_specs,
        out_shape=outs,
        scratch_shapes=[pltpu.VMEM((ny // 128, 2 * lines, 128), F32)] * 2,
        compiler_params=pltpu.CompilerParams(dimension_semantics=("arbitrary",)),
        name=f"spectral_{mode}_{len(basis)}",
    )(*args)
    return dict(zip(out_names, got))


def finish_call(plan, dots, iterate, basis, scal):
    ones = jnp.asarray(plan.ones)

    def kernel(*refs):
        out = refs[-1]
        sums = flow_sums(refs[0][...], refs[1])
        solved = solve_rows(sums, [r[...] for r in refs[3 + KRYLOV : 3 + 2 * KRYLOV]])
        value = refs[2][...]
        for i in range(KRYLOV):
            value = value + jnp.concatenate([solved[i]] * 2, axis=1) * refs[3 + i][...]
        out[...] = value

    shape = jax.ShapeDtypeStruct(iterate.shape, F32)
    return pl.pallas_call(kernel, out_shape=shape, name="finish")(dots, ones, iterate, *basis, *scal)


def values_call(plan, state):
    group, il, bq, ny = plan.group, plan.il, plan.bq, plan.ny
    if plan.direct:
        shape = jax.ShapeDtypeStruct((group, 2 * il + DOTS, bq), F32)
    else:
        shape = jax.ShapeDtypeStruct((2, ny, bq), F32)

    def kernel(ct, x, send):
        values = table_left(ct, x[...])
        for r in range(2):
            side = values[:, r * bq : (r + 1) * bq]
            if plan.direct:
                send[:, r * il : (r + 1) * il, :] = side.reshape(group, il, bq)
            else:
                send[r] = side
        if plan.direct:
            send[:, 2 * il :, :] = jnp.zeros((group, DOTS, bq), F32)

    return pl.pallas_call(kernel, out_shape=shape, name="values")(jnp.asarray(plan.ct), state)


def shards(start, forcing, taus):
    batch, _, kl, ny = start.shape
    group = lax.axis_size(AXES)
    plan = Plan(group, batch, kl, ny)
    il, bq = plan.il, plan.bq

    def swap(x):
        return lax.all_to_all(x, AXES, split_axis=0, concat_axis=0, tiled=True)

    def gather_dots(dots):
        return swap(jnp.broadcast_to(dots[None], (group,) + dots.shape))

    def move_out(sent, dots=None):
        if plan.direct:
            got = swap(sent)
            return got.reshape(group * (2 * il + DOTS), bq), None
        blocks = sent.reshape(2, group, il, bq).transpose(1, 0, 2, 3).reshape(group, 2 * il, bq)
        got = swap(blocks).reshape(group, 2, il, bq).transpose(1, 0, 2, 3)
        return got.reshape(2 * group, il * bq), None if dots is None else gather_dots(dots)

    def move_back(sent):
        if plan.direct:
            return swap(sent.reshape(group, 2 * il, bq))
        blocks = sent.reshape(2, group, il, bq).transpose(1, 0, 2, 3).reshape(group, 2 * il, bq)
        return swap(blocks).reshape(group, 2, il, bq).transpose(1, 0, 2, 3).reshape(2, ny, bq)

    def to_state(x):
        return x.transpose(3, 1, 0, 2).reshape(ny, 2 * bq)

    iterate, forced = to_state(start), to_state(forcing)
    field, _ = move_out(values_call(plan, iterate))
    sent, base = points_call(plan, "start", field)
    basis, solved = [], None
    for newton_step in range(NEWTON):
        got = spectral_call(plan, "residual", move_back(sent), taus, (iterate, forced), basis, solved)
        iterate = got.get("iterate", iterate)
        basis, basis_pts, scal = [], [], []
        for column in range(KRYLOV):
            field, dots = move_out(got["send"], got.get("dots"))
            sent, pts, rows = points_call(plan, "basis", field, dots, base, basis_pts)
            scal.append(rows)
            basis_pts.append(pts)
            got = spectral_call(
                plan, "krylov", move_back(sent), taus, (got["applied"],), basis, rows,
                emit=column < KRYLOV - 1,
            )
            basis.append(got["vector"])
        dots = gather_dots(got["dots"])
        if newton_step < NEWTON - 1:
            sent, base, solved = points_call(plan, "restart", None, dots, base, basis_pts, scal)
        else:
            iterate = finish_call(plan, dots, iterate, basis, scal)
    return iterate.reshape(ny, 2, batch, kl).transpose(2, 1, 3, 0)


def solution(mesh):
    return jax.shard_map(
        shards,
        mesh=mesh,
        in_specs=(
            P(None, None, AXES, None),
            P(None, None, AXES, None),
            P(AXES, None, None),
        ),
        out_specs=P(None, None, AXES, None),
        check_vma=False,
    )
```

```python
import math

import jax
import jax.numpy as jnp
import numpy as np
from jax import lax
from jax.experimental import pallas as pl
from jax.experimental.pallas import tpu as pltpu
from jax.sharding import PartitionSpec as P

NEWTON = 2
KRYLOV = 3
STRENGTH = 0.1
AXES = ("modes", "cheb")
F32 = jnp.float32
BF16 = jnp.bfloat16
GRANT = 20 * 2**20
DOTS = 8


def halves(table):
    table = np.asarray(table, np.float32)
    high = table.astype(BF16)
    low = (table - high.astype(np.float32)).astype(BF16)
    return np.stack([high, low])


def split(x):
    high = x.astype(BF16)
    return high, (x - high.astype(F32)).astype(BF16)


def mm(a, b):
    return lax.dot_general(a, b, (((1,), (0,)), ((), ())), preferred_element_type=F32)


def table_left(t_ref, x):
    high, low = split(x)
    return mm(t_ref[0], high) + (mm(t_ref[0], low) + mm(t_ref[1], high))


def table_right(x, t_ref):
    high, low = split(x)
    return mm(high, t_ref[0]) + (mm(low, t_ref[0]) + mm(high, t_ref[1]))


def least_squares(hessen, beta_norm):
    steps_count = len(hessen)
    matrix = [list(column) for column in hessen]
    target = [beta_norm] + [jnp.zeros_like(beta_norm)] * steps_count
    cosines = []
    sines = []
    for col in range(steps_count):
        column = matrix[col]
        for row in range(col):
            upper = cosines[row] * column[row] + sines[row] * column[row + 1]
            lower = cosines[row] * column[row + 1] - sines[row] * column[row]
            column[row] = upper
            column[row + 1] = lower
        radius = jnp.sqrt(column[col] * column[col] + column[col + 1] * column[col + 1])
        cosines.append(column[col] / radius)
        sines.append(column[col + 1] / radius)
        column[col] = radius
        target[col + 1] = -sines[col] * target[col]
        target[col] = cosines[col] * target[col]
    solved = [None] * steps_count
    for row in reversed(range(steps_count)):
        partial = target[row]
        for col in range(row + 1, steps_count):
            partial = partial - matrix[col][row] * solved[col]
        solved[row] = partial / matrix[row][row]
    return solved


SMALL = pltpu.CompilerParams(vmem_limit_bytes=GRANT)


class Plan:
    def __init__(self, group, batch, kl, ny):
        self.group, self.batch, self.kl, self.ny = group, batch, kl, ny
        self.il = ny // group
        self.bq = batch * kl
        self.j1 = 2 * group
        self.direct = self.il % 8 == 0 and self.bq % 128 == 0
        modes = kl * group
        points = 2 * modes
        spread = 1.0 / math.sqrt(modes * ny)
        tau = 2.0 * np.pi
        n, i = np.arange(ny)[:, None], np.arange(ny)[None, :]
        cheb = np.cos(tau / (4 * ny) * (n * (2 * i + 1) % (4 * ny)))
        self.ct = halves(cheb.T)
        self.cw = halves(cheb * (np.where(n == 0, 1.0, 2.0) / ny))
        d, j = np.arange(group)[None, :], np.arange(self.j1)[:, None]
        angle = tau / self.j1 * (d * j % self.j1)
        co, si = np.cos(angle), np.sin(angle)
        slope = 16.0 / modes * kl * d
        self.t1 = halves(np.block([
            [co, -si], [si, co], [-slope * si, -slope * co], [slope * co, -slope * si],
        ]))
        scale = STRENGTH / (spread * points)
        self.t4 = halves(scale * np.block([[co.T, si.T], [-si.T, co.T]]))
        q = np.arange(kl)
        twist = tau / points * (j * q[None, :] % points)
        slope_q = np.broadcast_to(16.0 / modes * q[None, :], twist.shape)
        self.tw = np.stack([
            np.tile(t, (1, batch)) for t in (np.cos(twist), np.sin(twist), slope_q)
        ]).astype(np.float32)
        weight = np.full((group, kl), 2.0 * spread)
        weight[0, 0] = spread
        self.wt = np.tile(weight, (2, batch)).astype(np.float32)
        inner = tau / kl * (q[:, None] * q[None, :] % kl)
        eye = np.eye(batch)
        self.b2 = halves(np.concatenate([np.kron(eye, np.cos(inner)), np.kron(eye, -np.sin(inner))], 0))
        self.b3 = halves(np.concatenate([np.kron(eye, np.cos(inner)), np.kron(eye, -np.sin(inner))], 1))
        self.ones = np.kron(eye, np.ones((kl, kl))).astype(np.float32)

    def tables(self):
        return [self.t1, self.tw, self.wt, self.b2, self.b3, self.t4, self.ones]


def flow_sums(dots, ones_ref):
    total = jnp.sum(dots, axis=0)
    return jnp.dot(total, ones_ref[...], precision=lax.Precision.HIGHEST, preferred_element_type=F32)


def new_column(sums, count):
    heads = [sums[i : i + 1] for i in range(count)]
    square = sums[count : count + 1]
    for head in heads:
        square = square - head * head
    return heads + [jnp.sqrt(square)]


def solve_rows(sums, scal):
    hessen = [[s[i : i + 1] for i in range(n + 2)] for n, s in enumerate(scal[1:])]
    hessen.append(new_column(sums, KRYLOV))
    return least_squares(hessen, scal[0][0:1])


def put_rows(ref, rows):
    ref[...] = jnp.zeros(ref.shape, F32)
    for index, row in enumerate(rows):
        ref[index : index + 1, :] = row


def points_call(plan, mode, field=None, dots=None, base=None, basis=(), scal=()):
    group, il, bq, j1 = plan.group, plan.il, plan.bq, plan.j1
    stride_in, stride_out = 2 * il + DOTS, 2 * il
    names, args = [], []

    def add(name, value):
        names.append(name)
        args.append(value)

    for name, value in zip(("t1", "tw", "wt", "b2", "b3", "t4", "ones"), plan.tables()):
        add(name, jnp.asarray(value))
    if field is not None:
        add("field", field)
    if dots is not None:
        add("dots", dots)
    if base is not None:
        add("base", base)
    for i, v in enumerate(basis):
        add(f"v{i}", v)
    for i, v in enumerate(scal):
        add(f"s{i}", v)
    pts_shape = jax.ShapeDtypeStruct((il, 2, j1, bq), F32)
    if plan.direct:
        send_shape = jax.ShapeDtypeStruct((group * stride_out, bq), F32)
    else:
        send_shape = jax.ShapeDtypeStruct((2 * group, il * bq), F32)
    outs = [send_shape, pts_shape]
    if mode != "start":
        outs.append(jax.ShapeDtypeStruct((DOTS, bq), F32))

    def kernel(*refs):
        ins = dict(zip(names, refs[: len(names)]))
        send, pts_out = refs[len(names)], refs[len(names) + 1]
        rows_out = refs[len(names) + 2] if mode != "start" else None

        def to_points():
            if plan.direct:
                sides = [
                    jnp.concatenate(
                        [ins["field"][pl.ds(r * il + i, group, stride=stride_in), :] for i in range(il)],
                        axis=1,
                    )
                    for r in range(2)
                ]
                x = jnp.concatenate(sides, axis=0)
            else:
                x = ins["field"][...]
            x = x * jnp.concatenate([ins["wt"][...]] * il, axis=1)
            z = table_left(ins["t1"], x)
            co, si, gq = ins["tw"][0], ins["tw"][1], ins["tw"][2]
            rows = []
            for i in range(il):
                part = z[:, i * bq : (i + 1) * bq]
                re, im = part[:j1], part[j1 : 2 * j1]
                sre = part[2 * j1 : 3 * j1] - gq * im
                sim = part[3 * j1 :] + gq * re
                for a, b in ((re, im), (sre, sim)):
                    rows.append(jnp.concatenate([a * co - b * si, a * si + b * co], axis=1))
            return table_right(jnp.concatenate(rows, axis=0), ins["b2"]).reshape(il, 2, j1, bq)

        if mode == "start":
            pts = to_points()
            pts_out[...] = pts
            product = pts[:, 0] * pts[:, 1]
        elif mode == "basis":
            if plan.direct:
                parts = ins["field"][...].reshape(group, stride_in, bq)[:, 2 * il :, :]
            else:
                parts = ins["dots"][...]
            sums = flow_sums(parts, ins["ones"])
            pts = to_points()
            if not basis:
                column = [jnp.sqrt(sums[0:1])]
                pts = pts * (-1.0 / column[0])
            else:
                column = new_column(sums, len(basis))
                for i in range(len(basis)):
                    pts = pts - column[i] * ins[f"v{i}"][...]
                pts = pts * (1.0 / column[-1])
            put_rows(rows_out, column)
            pts_out[...] = pts
            product = ins["base"][:, 0] * pts[:, 1] + pts[:, 0] * ins["base"][:, 1]
        else:
            sums = flow_sums(ins["dots"][...], ins["ones"])
            solved = solve_rows(sums, [ins[f"s{i}"][...] for i in range(KRYLOV)])
            pts = ins["base"][...]
            for i in range(KRYLOV):
                pts = pts + solved[i] * ins[f"v{i}"][...]
            put_rows(rows_out, solved)
            pts_out[...] = pts
            product = pts[:, 0] * pts[:, 1]
        part = table_right(product.reshape(il * j1, bq), ins["b3"])
        co, si = ins["tw"][0], ins["tw"][1]
        cols = []
        for i in range(il):
            re, im = part[i * j1 : (i + 1) * j1, :bq], part[i * j1 : (i + 1) * j1, bq:]
            cols.append(jnp.concatenate([re * co + im * si, im * co - re * si], axis=0))
        out = table_left(ins["t4"], jnp.concatenate(cols, axis=1))
        if plan.direct:
            for r in range(2):
                for i in range(il):
                    send[pl.ds(r * il + i, group, stride=stride_out), :] = out[
                        r * group : (r + 1) * group, i * bq : (i + 1) * bq
                    ]
        else:
            send[...] = out

    return pl.pallas_call(kernel, out_shape=outs, compiler_params=SMALL, name=f"points_{mode}_{len(basis)}")(*args)


def spectral_call(plan, mode, recv, taus, states, basis=(), scal=None, emit=True):
    group, il, bq, ny, kl = plan.group, plan.il, plan.bq, plan.ny, plan.kl
    wide = 2 * bq
    qb = min(8, kl)
    steps = kl // qb
    lines = wide
    names, args, specs = [], [], []

    def add(name, value):
        names.append(name)
        args.append(value)
        rank = value.ndim
        specs.append(pl.BlockSpec(value.shape, lambda s, rank=rank: (0,) * rank))

    add("recv", recv)
    add("ct", jnp.asarray(plan.ct))
    add("cw", jnp.asarray(plan.cw))
    for i, v in enumerate(states):
        add(f"x{i}", v)
    for i, v in enumerate(basis):
        add(f"v{i}", v)
    if scal is not None:
        add("scal", scal)
    first = not isinstance(taus, tuple)
    if first:
        names.append("taus")
        args.append(pltpu.with_memory_space_constraint(taus, pltpu.HBM))
        specs.append(pl.BlockSpec((qb, ny, ny), lambda s: (s, 0, 0)))
    else:
        for name, half in zip(("high", "low"), taus):
            names.append(name)
            args.append(half)
            specs.append(pl.BlockSpec(memory_space=pltpu.VMEM))

    state_shape = jax.ShapeDtypeStruct((ny, wide), F32)
    out_names, outs = [], []
    if mode == "residual":
        if basis:
            out_names.append("iterate")
            outs.append(state_shape)
    else:
        out_names.append("vector")
        outs.append(state_shape)
    if emit:
        out_names.append("applied")
        outs.append(state_shape)
        out_names.append("send")
        if plan.direct:
            outs.append(jax.ShapeDtypeStruct((group, 2 * il + DOTS, bq), F32))
        else:
            outs.append(jax.ShapeDtypeStruct((2, ny, bq), F32))
    if not (emit and plan.direct):
        out_names.append("dots")
        outs.append(jax.ShapeDtypeStruct((DOTS, bq), F32))
    out_specs = [
        pl.BlockSpec(o.shape, lambda s, rank=len(o.shape): (0,) * rank) for o in outs
    ]
    if first:
        out_names += ["high", "low"]
        outs += [pltpu.VMEM(taus.shape, BF16)] * 2
        out_specs += [pl.BlockSpec(memory_space=pltpu.VMEM)] * 2

    def kernel(*refs):
        ins = dict(zip(names, refs[: len(names)]))
        res = dict(zip(out_names, refs[len(names) : len(names) + len(outs)]))
        c_scr, m_scr = refs[len(names) + len(outs) :]
        step = pl.program_id(0)

        @pl.when(step == 0)
        def _():
            if plan.direct:
                sides = [
                    ins["recv"][:, r * il : (r + 1) * il, :].reshape(ny, bq) for r in range(2)
                ]
            else:
                sides = [ins["recv"][r] for r in range(2)]
            coef = table_left(ins["cw"], jnp.concatenate(sides, axis=1))
            if mode == "residual":
                coef = coef - ins["x1"][...]
            degree = lax.broadcasted_iota(jnp.int32, coef.shape, 0)
            coef = jnp.where(degree < ny - 2, coef, 0.0).T
            high = coef.astype(BF16).astype(F32)
            for h in range(ny // 128):
                c_scr[h, :lines, :] = high[:, h * 128 : (h + 1) * 128]
                c_scr[h, lines:, :] = (coef - high)[:, h * 128 : (h + 1) * 128]

        for t in range(qb):
            q = step * qb + t
            picked = pl.ds(q, 2 * lines // kl, stride=kl)
            rows = jnp.concatenate([c_scr[h, picked, :] for h in range(ny // 128)], axis=1).astype(BF16)
            dims = (((1,), (1,)), ((), ()))
            if first:
                high, low = split(ins["taus"][t])
                res["high"][q] = high
                res["low"][q] = low
            else:
                high, low = ins["high"][q], ins["low"][q]
            got = lax.dot_general(rows, high, dims, preferred_element_type=F32)
            got = got + lax.dot_general(rows, low, dims, preferred_element_type=F32)
            for h in range(ny // 128):
                m_scr[h, picked, :] = got[:, h * 128 : (h + 1) * 128]

        @pl.when(step == steps - 1)
        def _():
            mapped = jnp.concatenate(
                [m_scr[h, :lines, :] + m_scr[h, lines:, :] for h in range(ny // 128)], axis=1
            ).T

            def row(index):
                r = ins["scal"][index : index + 1, :]
                return jnp.concatenate([r, r], axis=1)

            vector = ins["x0"][...]
            if mode == "residual":
                if basis:
                    for i in range(len(basis)):
                        vector = vector + row(i) * ins[f"v{i}"][...]
                    res["iterate"][...] = vector
                others = []
            else:
                if not basis:
                    vector = vector * (-1.0 / row(0))
                else:
                    for i in range(len(basis)):
                        vector = vector - row(i) * ins[f"v{i}"][...]
                    vector = vector * (1.0 / row(len(basis)))
                res["vector"][...] = vector
                others = [ins[f"v{i}"][...] for i in range(len(basis))] + [vector]
            applied = vector + mapped
            lanes = []
            for other in others + [applied]:
                dot = jnp.sum(other * applied, axis=0, keepdims=True)
                lanes.append(dot[:, :bq] + dot[:, bq:])
            lanes += [jnp.zeros((1, bq), F32)] * (DOTS - len(lanes))
            dots = jnp.concatenate(lanes, axis=0)
            if emit:
                res["applied"][...] = applied
                values = table_left(ins["ct"], applied)
                for r in range(2):
                    side = values[:, r * bq : (r + 1) * bq]
                    if plan.direct:
                        res["send"][:, r * il : (r + 1) * il, :] = side.reshape(group, il, bq)
                    else:
                        res["send"][r] = side
            if emit and plan.direct:
                res["send"][:, 2 * il :, :] = jnp.broadcast_to(dots[None], (group, DOTS, bq))
            else:
                res["dots"][...] = dots

    got = pl.pallas_call(
        kernel,
        grid=(steps,),
        in_specs=specs,
        out_specs=out_specs,
        out_shape=outs,
        scratch_shapes=[pltpu.VMEM((ny // 128, 2 * lines, 128), F32)] * 2,
        compiler_params=pltpu.CompilerParams(
            dimension_semantics=("arbitrary",), vmem_limit_bytes=GRANT
        ),
        name=f"spectral_{mode}_{len(basis)}",
    )(*args)
    return dict(zip(out_names, got))


def finish_call(plan, dots, iterate, basis, scal):
    ones = jnp.asarray(plan.ones)

    def kernel(*refs):
        out = refs[-1]
        sums = flow_sums(refs[0][...], refs[1])
        solved = solve_rows(sums, [r[...] for r in refs[3 + KRYLOV : 3 + 2 * KRYLOV]])
        value = refs[2][...]
        for i in range(KRYLOV):
            value = value + jnp.concatenate([solved[i]] * 2, axis=1) * refs[3 + i][...]
        out[...] = value

    shape = jax.ShapeDtypeStruct(iterate.shape, F32)
    return pl.pallas_call(kernel, out_shape=shape, compiler_params=SMALL, name="finish")(dots, ones, iterate, *basis, *scal)


def values_call(plan, state):
    group, il, bq, ny = plan.group, plan.il, plan.bq, plan.ny
    if plan.direct:
        shape = jax.ShapeDtypeStruct((group, 2 * il + DOTS, bq), F32)
    else:
        shape = jax.ShapeDtypeStruct((2, ny, bq), F32)

    def kernel(ct, x, send):
        values = table_left(ct, x[...])
        for r in range(2):
            side = values[:, r * bq : (r + 1) * bq]
            if plan.direct:
                send[:, r * il : (r + 1) * il, :] = side.reshape(group, il, bq)
            else:
                send[r] = side
        if plan.direct:
            send[:, 2 * il :, :] = jnp.zeros((group, DOTS, bq), F32)

    return pl.pallas_call(kernel, out_shape=shape, compiler_params=SMALL, name="values")(jnp.asarray(plan.ct), state)


def shards(start, forcing, taus):
    batch, _, kl, ny = start.shape
    group = lax.axis_size(AXES)
    plan = Plan(group, batch, kl, ny)
    il, bq = plan.il, plan.bq

    def swap(x):
        return lax.all_to_all(x, AXES, split_axis=0, concat_axis=0, tiled=True)

    def gather_dots(dots):
        return swap(jnp.broadcast_to(dots[None], (group,) + dots.shape))

    def move_out(sent, dots=None):
        if plan.direct:
            got = swap(sent)
            return got.reshape(group * (2 * il + DOTS), bq), None
        blocks = sent.reshape(2, group, il, bq).transpose(1, 0, 2, 3).reshape(group, 2 * il, bq)
        got = swap(blocks).reshape(group, 2, il, bq).transpose(1, 0, 2, 3)
        return got.reshape(2 * group, il * bq), None if dots is None else gather_dots(dots)

    def move_back(sent):
        if plan.direct:
            return swap(sent.reshape(group, 2 * il, bq))
        blocks = sent.reshape(2, group, il, bq).transpose(1, 0, 2, 3).reshape(group, 2 * il, bq)
        return swap(blocks).reshape(group, 2, il, bq).transpose(1, 0, 2, 3).reshape(2, ny, bq)

    def to_state(x):
        return x.transpose(3, 1, 0, 2).reshape(ny, 2 * bq)

    iterate, forced = to_state(start), to_state(forcing)
    field, _ = move_out(values_call(plan, iterate))
    sent, base = points_call(plan, "start", field)
    basis, solved = [], None
    for newton_step in range(NEWTON):
        got = spectral_call(plan, "residual", move_back(sent), taus, (iterate, forced), basis, solved)
        iterate = got.get("iterate", iterate)
        if "high" in got:
            taus = (got["high"], got["low"])
        basis, basis_pts, scal = [], [], []
        for column in range(KRYLOV):
            field, dots = move_out(got["send"], got.get("dots"))
            sent, pts, rows = points_call(plan, "basis", field, dots, base, basis_pts)
            scal.append(rows)
            basis_pts.append(pts)
            got = spectral_call(
                plan, "krylov", move_back(sent), taus, (got["applied"],), basis, rows,
                emit=column < KRYLOV - 1,
            )
            basis.append(got["vector"])
        dots = gather_dots(got["dots"])
        if newton_step < NEWTON - 1:
            sent, base, solved = points_call(plan, "restart", None, dots, base, basis_pts, scal)
        else:
            iterate = finish_call(plan, dots, iterate, basis, scal)
    return iterate.reshape(ny, 2, batch, kl).transpose(2, 1, 3, 0)


def solution(mesh):
    return jax.shard_map(
        shards,
        mesh=mesh,
        in_specs=(
            P(None, None, AXES, None),
            P(None, None, AXES, None),
            P(AXES, None, None),
        ),
        out_specs=P(None, None, AXES, None),
        check_vma=False,
    )
```

```python
import math

import jax
import jax.numpy as jnp
import numpy as np
from jax import lax
from jax.experimental import pallas as pl
from jax.experimental.pallas import tpu as pltpu
from jax.sharding import PartitionSpec as P

NEWTON = 2
KRYLOV = 3
STRENGTH = 0.1
AXES = ("modes", "cheb")
F32 = jnp.float32
BF16 = jnp.bfloat16
GRANT = 20 * 2**20
DOTS = 8


def halves(table):
    table = np.asarray(table, np.float32)
    high = table.astype(BF16)
    low = (table - high.astype(np.float32)).astype(BF16)
    return np.stack([high, low])


def from_hbm(x):
    return pltpu.with_memory_space_constraint(x, pltpu.HBM)


def split(x):
    high = x.astype(BF16)
    return high, (x - high.astype(F32)).astype(BF16)


def mm(a, b):
    return lax.dot_general(a, b, (((1,), (0,)), ((), ())), preferred_element_type=F32)


def table_left(t_ref, x):
    high, low = split(x)
    return mm(t_ref[0], high) + (mm(t_ref[0], low) + mm(t_ref[1], high))


def table_right(x, t_ref):
    high, low = split(x)
    return mm(high, t_ref[0]) + (mm(low, t_ref[0]) + mm(high, t_ref[1]))


def least_squares(hessen, beta_norm):
    steps_count = len(hessen)
    matrix = [list(column) for column in hessen]
    target = [beta_norm] + [jnp.zeros_like(beta_norm)] * steps_count
    cosines = []
    sines = []
    for col in range(steps_count):
        column = matrix[col]
        for row in range(col):
            upper = cosines[row] * column[row] + sines[row] * column[row + 1]
            lower = cosines[row] * column[row + 1] - sines[row] * column[row]
            column[row] = upper
            column[row + 1] = lower
        radius = jnp.sqrt(column[col] * column[col] + column[col + 1] * column[col + 1])
        cosines.append(column[col] / radius)
        sines.append(column[col + 1] / radius)
        column[col] = radius
        target[col + 1] = -sines[col] * target[col]
        target[col] = cosines[col] * target[col]
    solved = [None] * steps_count
    for row in reversed(range(steps_count)):
        partial = target[row]
        for col in range(row + 1, steps_count):
            partial = partial - matrix[col][row] * solved[col]
        solved[row] = partial / matrix[row][row]
    return solved


SMALL = pltpu.CompilerParams(vmem_limit_bytes=GRANT)


class Plan:
    def __init__(self, group, batch, kl, ny):
        self.group, self.batch, self.kl, self.ny = group, batch, kl, ny
        self.il = ny // group
        self.bq = batch * kl
        self.j1 = 2 * group
        self.direct = self.il % 8 == 0 and self.bq % 128 == 0
        modes = kl * group
        points = 2 * modes
        spread = 1.0 / math.sqrt(modes * ny)
        tau = 2.0 * np.pi
        n, i = np.arange(ny)[:, None], np.arange(ny)[None, :]
        cheb = np.cos(tau / (4 * ny) * (n * (2 * i + 1) % (4 * ny)))
        self.ct = halves(cheb.T)
        self.cw = halves(cheb * (np.where(n == 0, 1.0, 2.0) / ny))
        d, j = np.arange(group)[None, :], np.arange(self.j1)[:, None]
        angle = tau / self.j1 * (d * j % self.j1)
        co, si = np.cos(angle), np.sin(angle)
        slope = 16.0 / modes * kl * d
        self.t1 = halves(np.block([
            [co, -si], [si, co], [-slope * si, -slope * co], [slope * co, -slope * si],
        ]))
        scale = STRENGTH / (spread * points)
        self.t4 = halves(scale * np.block([[co.T, si.T], [-si.T, co.T]]))
        q = np.arange(kl)
        twist = tau / points * (j * q[None, :] % points)
        slope_q = np.broadcast_to(16.0 / modes * q[None, :], twist.shape)
        self.tw = np.stack([
            np.tile(t, (1, batch)) for t in (np.cos(twist), np.sin(twist), slope_q)
        ]).astype(np.float32)
        weight = np.full((group, kl), 2.0 * spread)
        weight[0, 0] = spread
        self.wt = np.tile(weight, (2, batch)).astype(np.float32)
        inner = tau / kl * (q[:, None] * q[None, :] % kl)
        eye = np.eye(batch)
        self.b2 = halves(np.concatenate([np.kron(eye, np.cos(inner)), np.kron(eye, -np.sin(inner))], 0))
        self.b3 = halves(np.concatenate([np.kron(eye, np.cos(inner)), np.kron(eye, -np.sin(inner))], 1))
        self.ones = np.kron(eye, np.ones((kl, kl))).astype(np.float32)

    def tables(self):
        return [self.t1, self.tw, self.wt, self.b2, self.b3, self.t4, self.ones]


def over_modes(dots, ones_ref):
    return jnp.dot(dots, ones_ref[...], precision=lax.Precision.HIGHEST, preferred_element_type=F32)


def pack_dots(lanes, ones_ref, kl):
    bq = lanes[0].shape[1]
    lanes = lanes + [jnp.zeros((1, bq), F32)] * (DOTS - len(lanes))
    sums = over_modes(jnp.concatenate(lanes, axis=0), ones_ref)
    row_of = lax.broadcasted_iota(jnp.int32, sums.shape, 0)
    lane = lax.broadcasted_iota(jnp.int32, sums.shape, 1)
    return jnp.sum(jnp.where(lane % kl == row_of, sums, 0.0), axis=0, keepdims=True)


def flow_sums(rows, ones_ref, kl):
    total = jnp.broadcast_to(jnp.sum(rows, axis=0, keepdims=True), (DOTS, rows.shape[1]))
    row_of = lax.broadcasted_iota(jnp.int32, total.shape, 0)
    lane = lax.broadcasted_iota(jnp.int32, total.shape, 1)
    return over_modes(jnp.where(lane % kl == row_of, total, 0.0), ones_ref)


def new_column(sums, count):
    heads = [sums[i : i + 1] for i in range(count)]
    square = sums[count : count + 1]
    for head in heads:
        square = square - head * head
    return heads + [jnp.sqrt(square)]


def solve_rows(sums, scal):
    hessen = [[s[i : i + 1] for i in range(n + 2)] for n, s in enumerate(scal[1:])]
    hessen.append(new_column(sums, KRYLOV))
    return least_squares(hessen, scal[0][0:1])


def put_rows(ref, rows):
    ref[...] = jnp.zeros(ref.shape, F32)
    for index, row in enumerate(rows):
        ref[index : index + 1, :] = row


def points_call(plan, mode, field=None, dots=None, base=None, basis=(), scal=()):
    group, il, bq, j1 = plan.group, plan.il, plan.bq, plan.j1
    stride_in, stride_out = 2 * il + (mode == "basis"), 2 * il
    names, args = [], []

    def add(name, value):
        names.append(name)
        args.append(value)

    for name, value in zip(("t1", "tw", "wt", "b2", "b3", "t4", "ones"), plan.tables()):
        value = jnp.asarray(value)
        add(name, from_hbm(value) if mode == "start" else value)
    if field is not None:
        add("field", field)
    if dots is not None:
        add("dots", dots)
    if base is not None:
        add("base", base)
    for i, v in enumerate(basis):
        add(f"v{i}", v)
    for i, v in enumerate(scal):
        add(f"s{i}", v)
    pts_shape = jax.ShapeDtypeStruct((il, 2, j1, bq), F32)
    if plan.direct:
        send_shape = jax.ShapeDtypeStruct((group * stride_out, bq), F32)
    else:
        send_shape = jax.ShapeDtypeStruct((2 * group, il * bq), F32)
    outs = [send_shape, pts_shape]
    if mode != "start":
        outs.append(jax.ShapeDtypeStruct((DOTS, bq), F32))

    def kernel(*refs):
        ins = dict(zip(names, refs[: len(names)]))
        send, pts_out = refs[len(names)], refs[len(names) + 1]
        rows_out = refs[len(names) + 2] if mode != "start" else None

        def to_points():
            if plan.direct:
                sides = [
                    jnp.concatenate(
                        [ins["field"][pl.ds(r * il + i, group, stride=stride_in), :] for i in range(il)],
                        axis=1,
                    )
                    for r in range(2)
                ]
                x = jnp.concatenate(sides, axis=0)
            else:
                x = ins["field"][...]
            x = x * jnp.concatenate([ins["wt"][...]] * il, axis=1)
            z = table_left(ins["t1"], x)
            co, si, gq = ins["tw"][0], ins["tw"][1], ins["tw"][2]
            rows = []
            for i in range(il):
                part = z[:, i * bq : (i + 1) * bq]
                re, im = part[:j1], part[j1 : 2 * j1]
                sre = part[2 * j1 : 3 * j1] - gq * im
                sim = part[3 * j1 :] + gq * re
                for a, b in ((re, im), (sre, sim)):
                    rows.append(jnp.concatenate([a * co - b * si, a * si + b * co], axis=1))
            return table_right(jnp.concatenate(rows, axis=0), ins["b2"]).reshape(il, 2, j1, bq)

        if mode == "start":
            pts = to_points()
            pts_out[...] = pts
            product = pts[:, 0] * pts[:, 1]
        elif mode == "basis":
            if plan.direct:
                parts = ins["field"][pl.ds(2 * il, group, stride=stride_in), :]
            else:
                parts = ins["dots"][...]
            sums = flow_sums(parts, ins["ones"], plan.kl)
            pts = to_points()
            if not basis:
                column = [jnp.sqrt(sums[0:1])]
                pts = pts * (-1.0 / column[0])
            else:
                column = new_column(sums, len(basis))
                for i in range(len(basis)):
                    pts = pts - column[i] * ins[f"v{i}"][...]
                pts = pts * (1.0 / column[-1])
            put_rows(rows_out, column)
            pts_out[...] = pts
            product = ins["base"][:, 0] * pts[:, 1] + pts[:, 0] * ins["base"][:, 1]
        else:
            sums = flow_sums(ins["dots"][...], ins["ones"], plan.kl)
            solved = solve_rows(sums, [ins[f"s{i}"][...] for i in range(KRYLOV)])
            pts = ins["base"][...]
            for i in range(KRYLOV):
                pts = pts + solved[i] * ins[f"v{i}"][...]
            put_rows(rows_out, solved)
            pts_out[...] = pts
            product = pts[:, 0] * pts[:, 1]
        part = table_right(product.reshape(il * j1, bq), ins["b3"])
        co, si = ins["tw"][0], ins["tw"][1]
        cols = []
        for i in range(il):
            re, im = part[i * j1 : (i + 1) * j1, :bq], part[i * j1 : (i + 1) * j1, bq:]
            cols.append(jnp.concatenate([re * co + im * si, im * co - re * si], axis=0))
        out = table_left(ins["t4"], jnp.concatenate(cols, axis=1))
        if plan.direct:
            for r in range(2):
                for i in range(il):
                    send[pl.ds(r * il + i, group, stride=stride_out), :] = out[
                        r * group : (r + 1) * group, i * bq : (i + 1) * bq
                    ]
        else:
            send[...] = out

    return pl.pallas_call(kernel, out_shape=outs, compiler_params=SMALL, name=f"points_{mode}_{len(basis)}")(*args)


def spectral_call(plan, mode, recv, taus, states, basis=(), scal=None, emit=True):
    group, il, bq, ny, kl = plan.group, plan.il, plan.bq, plan.ny, plan.kl
    wide = 2 * bq
    qb = min(8, kl)
    steps = kl // qb
    lines = wide
    names, args, specs = [], [], []

    def add(name, value):
        names.append(name)
        args.append(value)
        rank = value.ndim
        specs.append(pl.BlockSpec(value.shape, lambda s, rank=rank: (0,) * rank))

    add("recv", recv)
    first = not isinstance(taus, tuple)
    for name, value in (("ct", plan.ct), ("cw", plan.cw), ("ones", plan.ones)):
        value = jnp.asarray(value)
        add(name, from_hbm(value) if first else value)
    for i, v in enumerate(states):
        add(f"x{i}", v)
    for i, v in enumerate(basis):
        add(f"v{i}", v)
    if scal is not None:
        add("scal", scal)
    if first:
        names.append("taus")
        args.append(from_hbm(taus))
        specs.append(pl.BlockSpec((qb, ny, ny), lambda s: (s, 0, 0)))
    else:
        for name, half in zip(("high", "low"), taus):
            names.append(name)
            args.append(half)
            specs.append(pl.BlockSpec(memory_space=pltpu.VMEM))

    state_shape = jax.ShapeDtypeStruct((ny, wide), F32)
    out_names, outs = [], []
    if mode == "residual":
        if basis:
            out_names.append("iterate")
            outs.append(state_shape)
    else:
        out_names.append("vector")
        outs.append(state_shape)
    if emit:
        out_names.append("applied")
        outs.append(state_shape)
        out_names.append("send")
        if plan.direct:
            outs.append(jax.ShapeDtypeStruct((group * (2 * il + 1), bq), F32))
        else:
            outs.append(jax.ShapeDtypeStruct((2, ny, bq), F32))
    if not (emit and plan.direct):
        out_names.append("dots")
        outs.append(jax.ShapeDtypeStruct((group, bq), F32))
    out_specs = [
        pl.BlockSpec(o.shape, lambda s, rank=len(o.shape): (0,) * rank) for o in outs
    ]
    if first:
        out_names += ["high", "low"]
        outs += [pltpu.VMEM(taus.shape, BF16)] * 2
        out_specs += [pl.BlockSpec(memory_space=pltpu.VMEM)] * 2

    def kernel(*refs):
        ins = dict(zip(names, refs[: len(names)]))
        res = dict(zip(out_names, refs[len(names) : len(names) + len(outs)]))
        c_scr, m_scr = refs[len(names) + len(outs) :]
        step = pl.program_id(0)

        @pl.when(step == 0)
        def _():
            if plan.direct:
                sides = [
                    ins["recv"][:, r * il : (r + 1) * il, :].reshape(ny, bq) for r in range(2)
                ]
            else:
                sides = [ins["recv"][r] for r in range(2)]
            coef = table_left(ins["cw"], jnp.concatenate(sides, axis=1))
            if mode == "residual":
                coef = coef - ins["x1"][...]
            degree = lax.broadcasted_iota(jnp.int32, coef.shape, 0)
            coef = jnp.where(degree < ny - 2, coef, 0.0).T
            high = coef.astype(BF16).astype(F32)
            for h in range(ny // 128):
                c_scr[h, :lines, :] = high[:, h * 128 : (h + 1) * 128]
                c_scr[h, lines:, :] = (coef - high)[:, h * 128 : (h + 1) * 128]

        for t in range(qb):
            q = step * qb + t
            picked = pl.ds(q, 2 * lines // kl, stride=kl)
            rows = jnp.concatenate([c_scr[h, picked, :] for h in range(ny // 128)], axis=1).astype(BF16)
            dims = (((1,), (1,)), ((), ()))
            if first:
                high, low = split(ins["taus"][t])
                res["high"][q] = high
                res["low"][q] = low
            else:
                high, low = ins["high"][q], ins["low"][q]
            got = lax.dot_general(rows, high, dims, preferred_element_type=F32)
            got = got + lax.dot_general(rows, low, dims, preferred_element_type=F32)
            for h in range(ny // 128):
                m_scr[h, picked, :] = got[:, h * 128 : (h + 1) * 128]

        @pl.when(step == steps - 1)
        def _():
            mapped = jnp.concatenate(
                [m_scr[h, :lines, :] + m_scr[h, lines:, :] for h in range(ny // 128)], axis=1
            ).T

            def row(index):
                r = ins["scal"][index : index + 1, :]
                return jnp.concatenate([r, r], axis=1)

            vector = ins["x0"][...]
            if mode == "residual":
                if basis:
                    for i in range(len(basis)):
                        vector = vector + row(i) * ins[f"v{i}"][...]
                    res["iterate"][...] = vector
                others = []
            else:
                if not basis:
                    vector = vector * (-1.0 / row(0))
                else:
                    for i in range(len(basis)):
                        vector = vector - row(i) * ins[f"v{i}"][...]
                    vector = vector * (1.0 / row(len(basis)))
                res["vector"][...] = vector
                others = [ins[f"v{i}"][...] for i in range(len(basis))] + [vector]
            applied = vector + mapped
            lanes = []
            for other in others + [applied]:
                dot = jnp.sum(other * applied, axis=0, keepdims=True)
                lanes.append(dot[:, :bq] + dot[:, bq:])
            dots = jnp.broadcast_to(pack_dots(lanes, ins["ones"], kl), (group, bq))
            if emit:
                res["applied"][...] = applied
                values = table_left(ins["ct"], applied)
                for r in range(2):
                    side = values[:, r * bq : (r + 1) * bq]
                    if plan.direct:
                        for e in range(group):
                            at = e * (2 * il + 1) + r * il
                            res["send"][at : at + il, :] = side[e * il : (e + 1) * il]
                    else:
                        res["send"][r] = side
            if emit and plan.direct:
                res["send"][pl.ds(2 * il, group, stride=2 * il + 1), :] = dots
            else:
                res["dots"][...] = dots

    got = pl.pallas_call(
        kernel,
        grid=(steps,),
        in_specs=specs,
        out_specs=out_specs,
        out_shape=outs,
        scratch_shapes=[pltpu.VMEM((ny // 128, 2 * lines, 128), F32)] * 2,
        compiler_params=pltpu.CompilerParams(
            dimension_semantics=("arbitrary",), vmem_limit_bytes=GRANT
        ),
        name=f"spectral_{mode}_{len(basis)}",
    )(*args)
    return dict(zip(out_names, got))


def finish_call(plan, dots, iterate, basis, scal):
    ones = jnp.asarray(plan.ones)

    def kernel(*refs):
        out = refs[-1]
        sums = flow_sums(refs[0][...], refs[1], plan.kl)
        solved = solve_rows(sums, [r[...] for r in refs[3 + KRYLOV : 3 + 2 * KRYLOV]])
        value = refs[2][...]
        for i in range(KRYLOV):
            value = value + jnp.concatenate([solved[i]] * 2, axis=1) * refs[3 + i][...]
        out[...] = value

    shape = jax.ShapeDtypeStruct(iterate.shape, F32)
    return pl.pallas_call(kernel, out_shape=shape, compiler_params=SMALL, name="finish")(dots, ones, iterate, *basis, *scal)


def values_call(plan, state):
    group, il, bq, ny = plan.group, plan.il, plan.bq, plan.ny
    if plan.direct:
        shape = jax.ShapeDtypeStruct((group, 2 * il, bq), F32)
    else:
        shape = jax.ShapeDtypeStruct((2, ny, bq), F32)

    def kernel(ct, x, send):
        values = table_left(ct, x[...])
        for r in range(2):
            side = values[:, r * bq : (r + 1) * bq]
            if plan.direct:
                send[:, r * il : (r + 1) * il, :] = side.reshape(group, il, bq)
            else:
                send[r] = side

    return pl.pallas_call(kernel, out_shape=shape, compiler_params=SMALL, name="values")(
        from_hbm(jnp.asarray(plan.ct)), state
    )


def shards(start, forcing, taus):
    batch, _, kl, ny = start.shape
    group = lax.axis_size(AXES)
    plan = Plan(group, batch, kl, ny)
    il, bq = plan.il, plan.bq

    def swap(x):
        return lax.all_to_all(x, AXES, split_axis=0, concat_axis=0, tiled=True)

    def gather_dots(dots):
        return swap(dots.reshape(group, 1, bq)).reshape(group, bq)

    def move_out(sent, dots=None):
        if plan.direct:
            if sent.ndim == 2:
                sent = sent.reshape(group, 1, -1)
            return swap(sent).reshape(-1, bq), None
        blocks = sent.reshape(2, group, il, bq).transpose(1, 0, 2, 3).reshape(group, 2 * il, bq)
        got = swap(blocks).reshape(group, 2, il, bq).transpose(1, 0, 2, 3)
        return got.reshape(2 * group, il * bq), None if dots is None else gather_dots(dots)

    def move_back(sent):
        if plan.direct:
            return swap(sent.reshape(group, 2 * il, bq))
        blocks = sent.reshape(2, group, il, bq).transpose(1, 0, 2, 3).reshape(group, 2 * il, bq)
        return swap(blocks).reshape(group, 2, il, bq).transpose(1, 0, 2, 3).reshape(2, ny, bq)

    def to_state(x):
        return x.transpose(3, 1, 0, 2).reshape(ny, 2 * bq)

    iterate, forced = to_state(start), to_state(forcing)
    field, _ = move_out(values_call(plan, iterate))
    sent, base = points_call(plan, "start", field)
    basis, solved = [], None
    for newton_step in range(NEWTON):
        got = spectral_call(plan, "residual", move_back(sent), taus, (iterate, forced), basis, solved)
        iterate = got.get("iterate", iterate)
        if "high" in got:
            taus = (got["high"], got["low"])
        basis, basis_pts, scal = [], [], []
        for column in range(KRYLOV):
            field, dots = move_out(got["send"], got.get("dots"))
            sent, pts, rows = points_call(plan, "basis", field, dots, base, basis_pts)
            scal.append(rows)
            basis_pts.append(pts)
            got = spectral_call(
                plan, "krylov", move_back(sent), taus, (got["applied"],), basis, rows,
                emit=column < KRYLOV - 1,
            )
            basis.append(got["vector"])
        dots = gather_dots(got["dots"])
        if newton_step < NEWTON - 1:
            sent, base, solved = points_call(plan, "restart", None, dots, base, basis_pts, scal)
        else:
            iterate = finish_call(plan, dots, iterate, basis, scal)
    return iterate.reshape(ny, 2, batch, kl).transpose(2, 1, 3, 0)


def solution(mesh):
    return jax.shard_map(
        shards,
        mesh=mesh,
        in_specs=(
            P(None, None, AXES, None),
            P(None, None, AXES, None),
            P(AXES, None, None),
        ),
        out_specs=P(None, None, AXES, None),
        check_vma=False,
    )
```
